32 devices in a mesh: groups: 2 (over x), frame: 8 (over z, y), band: 2 (over core).
Axes of the slice: x: 2, y: 2, z: 4, core: 2. Of those that a mesh axis runs over, the one named last changes fastest.
Arguments:
- hidden_in: bfloat16 [16, 1536, 1152], P(('groups', 'frame'), 'band'), parts along dimension 0, may hold values from -6 to 6
- latents: float32 [16, 192, 128], P(('groups', 'frame'), 'band'), parts along dimension 0, may hold values from -6 to 6
- fresh_noise: float32 [384, 128], P(('groups', 'band')), parts along dimension 0, may hold values from -6 to 6
- level_index: int32 [16], P(('groups', 'frame')), parts along dimension 0, may hold values from 1 to 31
- time_table: int32 [32], replicated, may hold values from 0 to 999, as said below
- frame_offset: int32 [2], P('groups'), parts along dimension 0, may hold values from 0 to 1023
- mod_table: float32 [3456], replicated, may hold values from -3 to 3
- time_weight: bfloat16 [128, 3456], replicated, may hold values from -0.5 to 0.5
- spatial_qkv: bfloat16 [1152, 1728], replicated, may hold values from -6 to 6
- spatial_out: bfloat16 [576, 1152], replicated, may hold values from -0.25 to 0.25
- temporal_qkv: bfloat16 [1152, 1728], replicated, may hold values from -6 to 6
- temporal_out: bfloat16 [576, 1152], replicated, may hold values from -0.25 to 0.25
- final_gain: float32 [1152], replicated, may hold values from 0.5 to 1.5
- out_weight: bfloat16 [1152, 16], replicated, may hold values from -0.1875 to 0.1875
Outputs:
- hidden_out: bfloat16 [16, 1536, 1152], P(('groups', 'frame'), 'band'), parts along dimension 0
- velocity: float32 [16, 192, 128], P(('groups', 'frame'), 'band'), parts along dimension 0
- next_latents: float32 [16, 192, 128], P(('groups', 'frame'), 'band'), parts along dimension 0
The draws below stay inside these ranges and needn't reach their ends.
There are 2 independent parts, one for each index of `groups`. The reference program is written for one: setup_inputs(seed, part) draws one part's arguments, and reference() takes and returns one part's arrays. A program takes and returns all parts, laid end to end along the dimension named above; an argument that names none is the same for every part. Nothing has to cross between parts.
Inputs may be any that keep to these rules, and one draw needn't show every extreme that they name: `time_table`: entries rise strictly along the table, from 0 at the first entry to 999 at the last.
All inputs are finite; a program needn't handle non-finite values.
Results may differ from the reference program's by a relative error of at most 0.025.
Values may be sent and summed in bfloat16 or wider, within the bound.
No kernel may reach another device: no remote copies, remote signals or barrier semaphores. Data moves between devices by JAX's collectives and lax.ppermute only.
A program may use at most 128 MiB of HBM per device.

```python
import math
import jax
import jax.numpy as jnp
from jax import lax

D = 1152
HEADS = 8
HEAD_SIZE = 72
TFREQ = 128
LCH = 16
FT = 1536
FRAMES = 8
TLEN = 32


def draw_time_table(key, part):
    chosen = jax.random.permutation(jax.random.fold_in(key, 11), 998)[:TLEN - 2] + 1
    middle = jnp.sort(chosen.astype(jnp.int32))
    return jnp.concatenate([jnp.zeros((1,), jnp.int32), middle, jnp.full((1,), 999, jnp.int32)])


def drawn_weight(key, salt):
    base = jax.random.normal(jax.random.fold_in(key, salt), (D, 3, HEADS, HEAD_SIZE), jnp.float32)
    base = jnp.clip(base, -6.0, 6.0) / math.sqrt(D)
    return base.reshape(D, 3 * HEADS * HEAD_SIZE).astype(jnp.bfloat16)


def draw_spatial_qkv(key, part):
    return drawn_weight(key, 21)


def draw_temporal_qkv(key, part):
    return drawn_weight(key, 37)


def draw_hidden_in(key, part):
    values = jnp.clip(jax.random.normal(jax.random.fold_in(key, 51), (FRAMES, FT, D), jnp.float32), -6.0, 6.0)
    return values.astype(jnp.bfloat16)


def set_ends(entries, own_key, least, high):
    longest = entries.shape.index(max(entries.shape))
    spots = []
    for shift in (0, 1):
        where = [jax.random.randint(jax.random.fold_in(own_key, axis), (), 0, length) for axis, length in enumerate(entries.shape)]
        where[longest] = (where[longest] + shift) % entries.shape[longest]
        spots.append(tuple(where))
    return entries.at[spots[0]].set(least).at[spots[1]].set(high)


def block_levels(rng, dims, shards, smallest, largest):
    def one(dim, parts):
        heights = jax.random.uniform(jax.random.fold_in(jax.random.fold_in(rng, 6), dim), (parts,), jnp.float32, smallest / len(shards), largest / len(shards))
        return jnp.repeat(jnp.exp(heights), dims[dim] // parts).reshape((-1,) + (1,) * (len(dims) - dim - 1))

    gain = one(*shards[0])
    for cut in shards[1:]:
        gain = gain * one(*cut)
    return gain


def scatter_about(stream_key, extent, deviation, reach, split=(), held_as=jnp.bfloat16):
    gain = block_levels(stream_key, extent, split, -0.22, 0.18) if split else 1.0
    result = jax.random.normal(stream_key, extent, jnp.float32) * deviation * gain
    return jnp.minimum(jnp.maximum(result, -reach), reach).astype(held_as)


def setup_inputs(seed: int = 0, part: int = 0) -> dict:
    splits = jax.random.split(jax.random.key(seed), 15)
    part_keys = jax.random.split(jax.random.fold_in(splits[14], part), 15)
    return {
        "hidden_in": draw_hidden_in(jax.random.fold_in(jax.random.fold_in(splits[14], part), 71), part),
        "latents": scatter_about(part_keys[1], (FRAMES, FT * LCH // 128, 128), 1.0, 6.0, ((0, 8), (1, 2)), jnp.float32),
        "fresh_noise": scatter_about(part_keys[2], (FT * LCH // 128, 128), 1.0, 6.0, ((0, 2),), jnp.float32),
        "level_index": set_ends(jax.random.randint(part_keys[3], (FRAMES,), 1, TLEN), jax.random.fold_in(part_keys[3], 1), 1, TLEN - 1).astype(jnp.int32),
        "time_table": draw_time_table(jax.random.fold_in(splits[14], 71), part),
        "frame_offset": jax.random.randint(part_keys[5], (1,), 0, 1024).astype(jnp.int32),
        "mod_table": scatter_about(splits[6], (3 * D,), 0.5, 3.0, (), jnp.float32),
        "time_weight": scatter_about(splits[7], (TFREQ, 3 * D), TFREQ ** -0.5, 0.5),
        "spatial_qkv": draw_spatial_qkv(jax.random.fold_in(splits[14], 71), part),
        "spatial_out": scatter_about(splits[9], (HEADS * HEAD_SIZE, D), (HEADS * HEAD_SIZE) ** -0.5, 0.25),
        "temporal_qkv": draw_temporal_qkv(jax.random.fold_in(splits[14], 71), part),
        "temporal_out": scatter_about(splits[11], (HEADS * HEAD_SIZE, D), (HEADS * HEAD_SIZE) ** -0.5, 0.25),
        "final_gain": jnp.clip(1.0 + 0.1 * jax.random.normal(splits[12], (D,), jnp.float32), 0.5, 1.5),
        "out_weight": scatter_about(splits[13], (D, LCH), D ** -0.5, 0.1875),
    }


epsilon = 1e-06

def layer_norm(values):
    average = lax.optimization_barrier(jnp.mean(values, axis=-1, keepdims=True))
    centred = values - average
    variance = lax.optimization_barrier(jnp.mean(centred * centred, axis=-1, keepdims=True))
    return centred * lax.rsqrt(variance + epsilon)

def sinusoid(position, feature_count, first_sine):
    half_width = feature_count // 2
    frequency = jnp.exp(-math.log(10000.0) * jnp.arange(half_width, dtype=jnp.float32) / half_width)
    angles = position.astype(jnp.float32)[:, None] * frequency[None, :]
    if first_sine:
        return jnp.concatenate([jnp.sin(angles), jnp.cos(angles)], axis=-1)
    return jnp.concatenate([jnp.cos(angles), jnp.sin(angles)], axis=-1)

def attend(query_rows, key_matrix_rows, value_matrix_rows):
    attention_scores = jnp.einsum('ubg,wbg->buw', query_rows.astype(jnp.float32), key_matrix_rows.astype(jnp.float32)) / math.sqrt(HEAD_SIZE)
    row_max = lax.optimization_barrier(jnp.max(attention_scores, axis=-1, keepdims=True))
    attention_weight = jnp.exp(attention_scores - row_max).astype(jnp.bfloat16)
    denominator = lax.optimization_barrier(jnp.sum(attention_weight.astype(jnp.float32), axis=-1))
    weighted_sum = jnp.einsum('leq,qlr->ler', attention_weight.astype(jnp.float32), value_matrix_rows.astype(jnp.float32))
    mixed = weighted_sum / denominator[:, :, None]
    return jnp.transpose(mixed, (1, 0, 2)).reshape(query_rows.shape[0], -1).astype(jnp.bfloat16)

def reference(hidden_in, latents, fresh_noise, level_index, time_table, frame_offset, mod_table, time_weight, spatial_qkv, spatial_out, temporal_qkv, temporal_out, final_gain, out_weight):
    frames, frame_tokens, model_width = hidden_in.shape
    attended = spatial_out.shape[0]
    head_count = attended // HEAD_SIZE
    now_steps = time_table[level_index]
    next_steps = time_table[level_index - 1]
    activated = jax.nn.silu(sinusoid(now_steps, TFREQ, False)).astype(jnp.bfloat16)
    modulation = mod_table[None, :] + jnp.dot(activated, time_weight, preferred_element_type=jnp.float32)
    shift_part = modulation[:, None, :model_width]
    scale_part = modulation[:, None, model_width:2 * model_width]
    gate_part = modulation[:, None, 2 * model_width:]
    inputs = hidden_in.astype(jnp.float32)
    normed = (layer_norm(inputs) * (1.0 + scale_part) + shift_part).astype(jnp.bfloat16)

    def spatial_frame(frame_rows):
        projected = jnp.dot(frame_rows, spatial_qkv, preferred_element_type=jnp.float32).astype(jnp.bfloat16)
        parted = projected.reshape(frame_tokens, 3, head_count, HEAD_SIZE)
        mixed = attend(parted[:, 0], parted[:, 1], parted[:, 2])
        return jnp.dot(mixed, spatial_out, preferred_element_type=jnp.float32)
    residual = inputs + gate_part * lax.map(spatial_frame, normed)
    placed = sinusoid(jnp.arange(frames, dtype=jnp.int32) + frame_offset[0], model_width, True)
    temporal_in = (residual + placed[:, None, :]).astype(jnp.bfloat16)
    projected = jnp.dot(temporal_in.reshape(frames * frame_tokens, model_width), temporal_qkv, preferred_element_type=jnp.float32).astype(jnp.bfloat16)
    parted = jnp.transpose(projected.reshape(frames, frame_tokens, 3, head_count, HEAD_SIZE), (1, 2, 0, 3, 4))
    mixed = jax.vmap(lambda column: attend(column[0], column[1], column[2]))(parted)
    temporal_mixed = jnp.transpose(mixed, (1, 0, 2)).reshape(frames * frame_tokens, attended)
    temporal_term = jnp.dot(temporal_mixed, temporal_out, preferred_element_type=jnp.float32).reshape(frames, frame_tokens, model_width)
    residual = residual + gate_part * temporal_term
    hidden_out = residual.astype(jnp.bfloat16)
    final_rows = (layer_norm(residual) * final_gain).astype(jnp.bfloat16)
    velocity = jnp.dot(final_rows.reshape(frames * frame_tokens, model_width), out_weight, preferred_element_type=jnp.float32)
    velocity = velocity.reshape(frames, frame_tokens * LCH // 128, 128)
    time_delta = (next_steps - now_steps).astype(jnp.float32) / 1000.0
    update = latents + time_delta[:, None, None] * velocity
    next_latents = jnp.concatenate([fresh_noise[None], update[:-1]], axis=0)
    return (hidden_out, velocity, next_latents)
```

```python
import functools
import math

import jax
import jax.numpy as jnp
from jax import lax
from jax.experimental import pallas as pl
from jax.experimental.pallas import tpu as pltpu
from jax.sharding import PartitionSpec as P


HEAD_SIZE = 72

VALUE_ROWS = 80
PADDED = 128
LANES = 128
QUERY_BLOCK = 256

epsilon = 1e-06
scale_of_scores = 1.0 / math.sqrt(HEAD_SIZE)

WHOLE = pl.BlockSpec(memory_space=pltpu.VMEM)
SCALARS = pl.BlockSpec(memory_space=pltpu.SMEM)
REMAIN = pl.BlockSpec(memory_space=pltpu.HBM)
PARAMS = pltpu.CompilerParams(vmem_limit_bytes=24 * 1024 * 1024)
ACROSS = (((1,), (1,)), ((), ()))


def round_up(value, multiple):
    return (value + multiple - 1) // multiple * multiple


def from_behind(value, axis, steps):
    count = lax.axis_size(axis)
    initial, last = (max(0, -steps), min(count, count - steps))
    return lax.ppermute(value, axis, [(source, source + steps) for source in range(initial, last)])


def normalized(values):
    average = jnp.mean(values, axis=-1, keepdims=True)
    centred = values - average
    variance = jnp.mean(centred * centred, axis=-1, keepdims=True)
    return centred * lax.rsqrt(variance + epsilon)


def padded_rows(rows, total, first_fill):
    columns = rows.shape[1]
    fill = jnp.zeros((total - rows.shape[0], columns), jnp.float32)
    if first_fill:
        fill = jnp.where(lax.broadcasted_iota(jnp.int32, fill.shape, 0) == 0, 1.0, 0.0)
    return jnp.concatenate([rows, fill], axis=0)


def as_query(rows):
    return padded_rows(rows * scale_of_scores, PADDED, False).astype(jnp.bfloat16)


def as_key(rows):
    return jnp.transpose(padded_rows(rows, PADDED, False)).astype(jnp.bfloat16)


def as_value(rows):
    return padded_rows(rows, VALUE_ROWS, True).astype(jnp.bfloat16)


def sinusoid_row(position, width, half, sine_first):
    index = lax.broadcasted_iota(jnp.int32, (1, width), 1)
    place = jnp.where(index < half, index, index - half).astype(jnp.float32)
    angles = position * jnp.exp(-math.log(10000.0) * place / half)
    first, second = (jnp.sin(angles), jnp.cos(angles))
    if not sine_first:
        first, second = (second, first)
    return jnp.where(index < half, first, second)


def cost(microseconds):
    return pl.CostEstimate(
        flops=int(microseconds * 1e9), transcendentals=0, bytes_accessed=1024 * 1024
    )


def in_hbm(*arrays):
    return tuple(pltpu.with_memory_space_constraint(array, pltpu.HBM) for array in arrays)


def start_all(copies):
    for copy in copies:
        copy.start()
    return copies


def keys_values_kernel(
    level, table, offset, frame, hidden_far, mod_table, time_far, weight_far,
    keys, values, normed, modulation, placed,
    hidden, time_weight, weight, sems,
):
    rows_total, width = hidden.shape
    head_count = keys.shape[0]
    attended = head_count * HEAD_SIZE
    time_copy = pltpu.make_async_copy(time_far, time_weight, sems.at[0])
    hidden_copy = pltpu.make_async_copy(hidden_far, hidden, sems.at[1])
    weight_copies = [
        pltpu.make_async_copy(
            weight_far.at[pl.ds((1 + part) * attended, attended), :],
            weight.at[pl.ds(part * attended, attended), :],
            sems.at[2 + part],
        )
        for part in range(2)
    ]
    start_all([time_copy, hidden_copy] + weight_copies)
    now = table[level[0]].astype(jnp.float32)
    frequencies = time_weight.shape[0]
    embedded = sinusoid_row(now, frequencies, frequencies // 2, False)
    activated = (embedded * (1.0 / (1.0 + jnp.exp(-embedded)))).astype(jnp.bfloat16)
    spread = jnp.broadcast_to(activated.astype(jnp.float32), (16, frequencies)).astype(jnp.bfloat16)
    placed[...] = sinusoid_row(
        (frame[0] + offset[0]).astype(jnp.float32), width, width // 2, True
    )
    time_copy.wait()
    projected = jnp.dot(spread, time_weight[...], preferred_element_type=jnp.float32)
    modulation[...] = mod_table[...] + projected[:1, :]
    shift = modulation[:, :width]
    scale = 1.0 + modulation[:, width : 2 * width]
    hidden_copy.wait()
    for start in range(0, rows_total, QUERY_BLOCK):
        span = slice(start, start + QUERY_BLOCK)
        block = hidden[span, :].astype(jnp.float32)
        normed[span, :] = (normalized(block) * scale + shift).astype(jnp.bfloat16)
        if start == 0:
            weight_copies[0].wait()
            weight_copies[1].wait()
        turned = lax.dot_general(
            weight[...], normed[span, :], ACROSS, preferred_element_type=jnp.float32
        )
        for head in range(head_count):
            first = head * HEAD_SIZE
            keys[head, span, :] = as_key(turned[first : first + HEAD_SIZE, :])
            first += attended
            values[head, :, span] = as_value(turned[first : first + HEAD_SIZE, :])


def keys_and_values(level, table, offset, frame, hidden, mod_table, time_weight, weight, head_count):
    rows, width = hidden.shape
    hidden, time_weight, weight = in_hbm(hidden, time_weight, weight)
    return pl.pallas_call(
        keys_values_kernel,
        out_shape=(
            jax.ShapeDtypeStruct((head_count, rows, PADDED), jnp.bfloat16),
            jax.ShapeDtypeStruct((head_count, VALUE_ROWS, rows), jnp.bfloat16),
            jax.ShapeDtypeStruct((rows, width), jnp.bfloat16),
            jax.ShapeDtypeStruct(mod_table.shape, jnp.float32),
            jax.ShapeDtypeStruct((1, width), jnp.float32),
        ),
        in_specs=[SCALARS] * 4 + [REMAIN, WHOLE, REMAIN, REMAIN],
        out_specs=(WHOLE,) * 5,
        scratch_shapes=[
            pltpu.VMEM(hidden.shape, jnp.bfloat16),
            pltpu.VMEM(time_weight.shape, jnp.bfloat16),
            pltpu.VMEM((2 * head_count * HEAD_SIZE, width), jnp.bfloat16),
            pltpu.SemaphoreType.DMA((4,)),
        ],
        compiler_params=PARAMS,
        cost_estimate=cost(5),
        name="keys_and_values",
    )(level, table, offset, frame, hidden, mod_table, time_weight, weight)


def queries_kernel(normed, weight_far, queries, weight, sems):
    head_count = queries.shape[0]
    attended = head_count * HEAD_SIZE
    copy = pltpu.make_async_copy(weight_far.at[pl.ds(0, attended), :], weight, sems.at[0])
    copy.start()
    copy.wait()
    for start in range(0, normed.shape[0], QUERY_BLOCK):
        span = slice(start, start + QUERY_BLOCK)
        turned = lax.dot_general(
            weight[...], normed[span, :], ACROSS, preferred_element_type=jnp.float32
        )
        for head in range(head_count):
            first = head * HEAD_SIZE
            queries[head, :, span] = as_query(turned[first : first + HEAD_SIZE, :])


def project_queries(normed, weight, head_count):
    rows, width = normed.shape
    return pl.pallas_call(
        queries_kernel,
        out_shape=jax.ShapeDtypeStruct((head_count, PADDED, rows), jnp.bfloat16),
        in_specs=[WHOLE, REMAIN],
        out_specs=WHOLE,
        scratch_shapes=[
            pltpu.VMEM((head_count * HEAD_SIZE, width), jnp.bfloat16),
            pltpu.SemaphoreType.DMA((1,)),
        ],
        compiler_params=PARAMS,
        cost_estimate=cost(3),
        name="project_queries",
    )(normed, *in_hbm(weight))


def turn_back(turned, rows, attended):
    for start in range(0, attended, LANES):
        rows[:, start : start + LANES] = jnp.transpose(
            turned[start : start + LANES, :]
        ).astype(jnp.bfloat16)


def share_out(total):
    return total[:HEAD_SIZE, :] / total[HEAD_SIZE : HEAD_SIZE + 1, :]


def attend_kernel(
    first, resident, slots,
    frame, hidden_far, queries_in, keys_in, values_in, other_keys_in, other_values_in, weight_far,
    modulation, placed,
    residual_far, *refs,
):
    outs = max(slots, 1)
    temporal_far = refs[:outs]
    scores_a, scores_b, turned, rows, hidden, weight, residual, temporal_in, sems, *loaded = refs[outs:]
    count, width = residual.shape
    head_count = queries_in.shape[0]
    attended = head_count * HEAD_SIZE
    half = keys_in.shape[1]
    near = (queries_in, keys_in, values_in, other_keys_in, other_values_in)
    if not resident:
        far = (queries_in.at[:, :, pl.ds(first, count)],) + near[1:]
        near = loaded

        def head_copies(head):
            return [
                pltpu.make_async_copy(
                    source.at[head], target.at[head], sems.at[2 + head * len(near) + place]
                )
                for place, (source, target) in enumerate(zip(far, near))
            ]

        for head in range(head_count):
            start_all(head_copies(head))
    hidden_copy = pltpu.make_async_copy(
        hidden_far.at[pl.ds(first, count), :], hidden, sems.at[0]
    )
    weight_copy = pltpu.make_async_copy(weight_far, weight, sems.at[1])
    start_all([hidden_copy, weight_copy])
    queries, keys, values, other_keys, other_values = near
    stored = 2 + len(loaded) * head_count
    begin = first if resident else 0
    turned[attended:, :] = jnp.zeros((turned.shape[0] - attended, QUERY_BLOCK), jnp.float32)
    stores = []
    for start in range(0, count, QUERY_BLOCK):
        span = slice(begin + start, begin + start + QUERY_BLOCK)

        def one(head, scores):
            query = queries[head, :, span]
            own = jnp.dot(keys[head], query, preferred_element_type=jnp.float32)
            scores[:half, :] = own
            top = jnp.max(own, axis=0, keepdims=True)
            other = jnp.dot(other_keys[head], query, preferred_element_type=jnp.float32)
            scores[half:, :] = other
            top = jnp.maximum(top, jnp.max(other, axis=0, keepdims=True))
            weights = jnp.exp(scores[:half, :] - top).astype(jnp.bfloat16)
            total = jnp.dot(values[head], weights, preferred_element_type=jnp.float32)
            weights = jnp.exp(scores[half:, :] - top).astype(jnp.bfloat16)
            total += jnp.dot(other_values[head], weights, preferred_element_type=jnp.float32)
            turned[pl.ds(pl.multiple_of(head * HEAD_SIZE, 8), HEAD_SIZE), :] = share_out(total)

        def pair(index, carry):
            if start == 0 and not resident:
                for head in (2 * index, 2 * index + 1):
                    for copy in head_copies(head):
                        copy.wait()
            one(2 * index, scores_a)
            one(2 * index + 1, scores_b)
            return carry

        lax.fori_loop(0, head_count // 2, pair, 0)
        turn_back(turned, rows, attended)
        if start == 0:
            hidden_copy.wait()
            weight_copy.wait()
        gate = modulation[:, 2 * width :]
        step = QUERY_BLOCK // 2
        for part in range(0, QUERY_BLOCK, step):
            span = slice(start + part, start + part + step)
            term = jnp.dot(
                rows[part : part + step, :attended], weight[...],
                preferred_element_type=jnp.float32,
            )
            kept = hidden[span, :].astype(jnp.float32) + gate * term
            residual[span, :] = kept
            temporal_in[span, :] = (kept + placed[...]).astype(jnp.bfloat16)
            window = pl.ds(start + part, step)
            moves = [(residual.at[window, :], residual_far.at[window, :])]
            if not slots:
                moves.append((temporal_in.at[window, :], temporal_far[0].at[window, :]))
            stores += start_all(
                [
                    pltpu.make_async_copy(source, target, sems.at[stored + len(stores) + place])
                    for place, (source, target) in enumerate(moves)
                ]
            )
    share = count // outs
    for slot in range(slots):
        window = pl.ds(pl.multiple_of(lax.bitwise_xor(frame[0], slot) * share, 16), share)
        copy = pltpu.make_async_copy(
            temporal_in.at[window, :], temporal_far[slot], sems.at[stored + len(stores)]
        )
        copy.start()
        stores.append(copy)
    for copy in stores:
        copy.wait()


def attend(first, count, resident, slots, frame, hidden, projected, other, out_weight, modulation, placed):
    queries, keys, values = projected
    head_count = queries.shape[0]
    width = hidden.shape[1]
    attended = out_weight.shape[0]
    deep = round_up(attended, LANES)
    near = WHOLE if resident else REMAIN
    loaded = ()
    hidden, out_weight = in_hbm(hidden, out_weight)
    if not resident:
        queries, keys, values, *other = in_hbm(queries, keys, values, *other)
        loaded = tuple(
            pltpu.VMEM(shape, jnp.bfloat16)
            for shape in ((head_count, PADDED, count), keys.shape, values.shape, keys.shape, values.shape)
        )
    sem_count = 2 + len(loaded) * head_count + 4 * (count // QUERY_BLOCK) + slots
    outs = max(slots, 1)
    return pl.pallas_call(
        functools.partial(attend_kernel, first, resident, slots),
        out_shape=(
            pltpu.HBM((count, width), jnp.float32),
            *[pltpu.HBM((count // outs, width), jnp.bfloat16)] * outs,
        ),
        in_specs=[SCALARS, REMAIN] + [near] * 5 + [REMAIN] + [WHOLE] * 2,
        out_specs=(REMAIN,) * (1 + outs),
        scratch_shapes=[
            pltpu.VMEM((2 * keys.shape[1], QUERY_BLOCK), jnp.float32),
            pltpu.VMEM((2 * keys.shape[1], QUERY_BLOCK), jnp.float32),
            pltpu.VMEM((deep, QUERY_BLOCK), jnp.float32),
            pltpu.VMEM((QUERY_BLOCK, deep), jnp.bfloat16),
            pltpu.VMEM((count, width), jnp.bfloat16),
            pltpu.VMEM(out_weight.shape, jnp.bfloat16),
            pltpu.VMEM((count, width), jnp.float32),
            pltpu.VMEM((count, width), jnp.bfloat16),
            pltpu.SemaphoreType.DMA((sem_count,)),
            *loaded,
        ],
        compiler_params=PARAMS,
        cost_estimate=cost(0.028 * count),
        name="attend",
    )(frame, hidden, queries, keys, values, *other, out_weight, modulation, placed)


def temporal_kernel(group, tokens, parts, *refs):
    gathered, weight_far, mixed = (refs[:parts], refs[parts], refs[-6 - parts : -6])
    weight, turned, bias, turned_out, rows, sems = refs[-6:]
    frames, share, width = gathered[0].shape
    attended = mixed[0].shape[2]
    head_count = attended // HEAD_SIZE
    count = bias.shape[0]
    weight_copies = start_all(
        [
            pltpu.make_async_copy(
                weight_far.at[pl.ds(part * attended, attended), :],
                weight.at[pl.ds(part * attended, attended), :],
                sems.at[part],
            )
            for part in range(3)
        ]
    )
    own = lax.rem(lax.broadcasted_iota(jnp.int32, (count, count), 0), tokens)
    other = lax.rem(lax.broadcasted_iota(jnp.int32, (count, count), 1), tokens)
    bias[...] = jnp.where(own == other, 0.0, -1e30)
    turned_out[attended:, :] = jnp.zeros((turned_out.shape[0] - attended, count), jnp.float32)
    for start in range(0, share, group):
        block = jnp.concatenate(
            [part[:, start : start + group, :].reshape(frames * group, width) for part in gathered],
            axis=0,
        )
        for part in range(3):
            if start == 0:
                weight_copies[part].wait()
            span = slice(part * attended, (part + 1) * attended)
            turned[span, :] = lax.dot_general(
                weight[span, :], block, ACROSS, preferred_element_type=jnp.float32
            )
        for head in range(head_count):
            query, key, value = (
                turned[part * attended + head * HEAD_SIZE : part * attended + (head + 1) * HEAD_SIZE, :]
                for part in range(3)
            )
            scores = jnp.dot(as_key(key), as_query(query), preferred_element_type=jnp.float32)
            scores = scores + bias[...]
            top = jnp.max(scores, axis=0, keepdims=True)
            weights = jnp.exp(scores - top).astype(jnp.bfloat16)
            total = jnp.dot(as_value(value), weights, preferred_element_type=jnp.float32)
            turned_out[head * HEAD_SIZE : (head + 1) * HEAD_SIZE, :] = share_out(total)
        turn_back(turned_out, rows, attended)
        for place, part in enumerate(mixed):
            span = slice(place * frames * group, (place + 1) * frames * group)
            part[:, start : start + group, :] = rows[span, :attended].reshape(frames, group, attended)


def mix_frames(gathered, weight, attended, after):
    parts = len(gathered)
    given = gathered[0].shape
    frames, share, width = given
    whole = parts * frames
    group = QUERY_BLOCK // whole if QUERY_BLOCK % whole == 0 else 0
    shape, tokens = given, group
    if group == 0 or group % 16 or share % group:
        shape, group, tokens = ((1, frames * share, width), frames * share, share)
    count = parts * shape[0] * group
    deep = round_up(attended, LANES)
    mixed = pl.pallas_call(
        functools.partial(temporal_kernel, group, tokens, parts),
        out_shape=(pltpu.HBM(shape[:2] + (attended,), jnp.bfloat16),) * parts,
        in_specs=[WHOLE] * parts + [REMAIN] * (1 + len(after)),
        out_specs=(WHOLE,) * parts,
        scratch_shapes=[
            pltpu.VMEM(weight.shape, jnp.bfloat16),
            pltpu.VMEM((weight.shape[0], count), jnp.float32),
            pltpu.VMEM((count, count), jnp.float32),
            pltpu.VMEM((deep, count), jnp.float32),
            pltpu.VMEM((count, deep), jnp.bfloat16),
            pltpu.SemaphoreType.DMA((3,)),
        ],
        compiler_params=PARAMS,
        cost_estimate=cost(0.025 * count),
        name="mix_frames",
    )(*[part.reshape(shape) for part in gathered], *in_hbm(weight, *after))
    return [part.reshape(given[:2] + (attended,)) for part in mixed]


def finish_kernel(
    first, parts, level, table, frame, residual_far, weight_far, modulation, gain, out_weight,
    latents_far, *refs,
):
    returned = refs[:parts]
    hidden_far, velocity_far, update_far, residual, weight, latents, hidden, velocity, update, mixed, sems = refs[-11:]
    count, width = residual.shape
    channels = out_weight.shape[0]
    fold = LANES // channels
    lines = pl.ds(first // fold, count // fold)
    weight_copy = pltpu.make_async_copy(weight_far, weight, sems.at[0])
    residual_copy = pltpu.make_async_copy(residual_far, residual, sems.at[1])
    latents_copy = pltpu.make_async_copy(latents_far.at[lines, :], latents, sems.at[2])
    start_all([weight_copy, residual_copy, latents_copy])
    spread = lax.rem(lax.broadcasted_iota(jnp.int32, (LANES, channels), 0), channels)
    spread = jnp.where(
        spread == lax.broadcasted_iota(jnp.int32, (LANES, channels), 1), 1.0, 0.0
    ).astype(jnp.bfloat16)
    repeated = jnp.dot(spread, out_weight[...], preferred_element_type=jnp.float32)
    repeated = repeated.astype(jnp.bfloat16)
    for slot, part in enumerate(returned):
        share = part.shape[0]
        where = lax.bitwise_xor(frame[0], slot) * share if parts > 1 else 0
        mixed[pl.ds(pl.multiple_of(where, 16), share), :] = part[...]
    weight_copy.wait()
    residual_copy.wait()
    stores = []
    for start in range(0, count, QUERY_BLOCK):
        span = slice(start, start + QUERY_BLOCK)
        term = jnp.dot(mixed[span, :], weight[...], preferred_element_type=jnp.float32)
        block = residual[span, :] + modulation[:, 2 * width :] * term
        hidden[span, :] = block.astype(jnp.bfloat16)
        copy = pltpu.make_async_copy(
            hidden.at[pl.ds(start, QUERY_BLOCK), :],
            hidden_far.at[pl.ds(first + start, QUERY_BLOCK), :],
            sems.at[5 + len(stores)],
        )
        copy.start()
        stores.append(copy)
        final_rows = (normalized(block) * gain[...]).astype(jnp.bfloat16)
        wide = lax.dot_general(final_rows, repeated, ACROSS, preferred_element_type=jnp.float32)
        row = lax.rem(lax.broadcasted_iota(jnp.int32, (QUERY_BLOCK, LANES), 0), fold)
        lane = lax.broadcasted_iota(jnp.int32, (QUERY_BLOCK, LANES), 1) // channels
        picked = jnp.where(row == lane, wide, 0.0).reshape(QUERY_BLOCK // fold, fold, LANES)
        velocity[start // fold : (start + QUERY_BLOCK) // fold, :] = jnp.sum(picked, axis=1)
    now = table[level[0]]
    following = table[level[0] - 1]
    delta = (following - now).astype(jnp.float32) / 1000.0
    latents_copy.wait()
    update[...] = (latents[...] + delta * velocity[...]).astype(jnp.bfloat16)
    stores += start_all(
        [
            pltpu.make_async_copy(velocity, velocity_far.at[lines, :], sems.at[3]),
            pltpu.make_async_copy(update, update_far.at[lines, :], sems.at[4]),
        ]
    )
    for copy in stores:
        copy.wait()


def finish(first, so_far, level, table, frame, residual, mixed, weight, modulation, gain, out_weight, latents, tokens):
    count, width = residual.shape
    lines = count * out_weight.shape[0] // LANES
    known = 9 + len(mixed)
    residual, weight, latents = in_hbm(residual, weight, latents)
    return pl.pallas_call(
        functools.partial(finish_kernel, first, len(mixed)),
        out_shape=(
            pltpu.HBM((tokens, width), jnp.bfloat16),
            pltpu.HBM(latents.shape, jnp.float32),
            pltpu.HBM(latents.shape, jnp.bfloat16),
        ),
        in_specs=[SCALARS] * 3
        + [REMAIN] * 2
        + [WHOLE] * 3
        + [REMAIN]
        + [WHOLE] * len(mixed)
        + [REMAIN] * len(so_far),
        out_specs=(REMAIN,) * 3,
        scratch_shapes=[
            pltpu.VMEM((count, width), jnp.float32),
            pltpu.VMEM(weight.shape, jnp.bfloat16),
            pltpu.VMEM((lines, LANES), jnp.float32),
            pltpu.VMEM((count, width), jnp.bfloat16),
            pltpu.VMEM((lines, LANES), jnp.float32),
            pltpu.VMEM((lines, LANES), jnp.bfloat16),
            pltpu.VMEM((count, weight.shape[0]), jnp.bfloat16),
            pltpu.SemaphoreType.DMA((5 + count // QUERY_BLOCK,)),
        ],
        input_output_aliases={known + place: place for place in range(len(so_far))},
        compiler_params=PARAMS,
        cost_estimate=cost(0.012 * count),
        name="finish",
    )(level, table, frame, residual, weight, modulation, gain, out_weight, latents, *mixed, *so_far)


FIRST_BLOCKS = 1
PERMUTED = (1,)


def chunks_of(tokens, peers):
    least = round_up(QUERY_BLOCK, 16 * peers)
    head = FIRST_BLOCKS * least
    if least % QUERY_BLOCK or tokens % least or head >= tokens:
        return [(0, tokens)]
    return [(0, head), (head, tokens - head)]


def by_permutes(place, peers):
    return place in PERMUTED and peers & (peers - 1) == 0


def exchange(parts, peers):
    if len(parts) == 1:
        return [lax.all_to_all(parts[0], "frame", 0, 0, tiled=True)]
    arrived = [parts[0]]
    for slot in range(1, peers):
        pairs = [(index, index ^ slot) for index in range(peers)]
        arrived.append(lax.ppermute(parts[slot], "frame", pairs))
    return arrived


def steps(
    hidden_in,
    latents,
    fresh_noise,
    level_index,
    time_table,
    frame_offset,
    mod_table,
    time_weight,
    spatial_qkv,
    spatial_out,
    temporal_qkv,
    temporal_out,
    final_gain,
    out_weight,
):
    tokens = hidden_in.shape[1]
    attended = spatial_out.shape[0]
    head_count = attended // HEAD_SIZE
    peers = lax.axis_size("frame")
    hidden = hidden_in[0]
    frame = lax.axis_index("frame").astype(jnp.int32).reshape(1)
    spatial_turned = jnp.transpose(spatial_qkv)
    temporal_turned = jnp.transpose(temporal_qkv)
    keys, values, normed, modulation, placed = keys_and_values(
        level_index, time_table, frame_offset, frame, hidden, mod_table[None, :],
        time_weight, spatial_turned, head_count,
    )
    swap = [(0, 1), (1, 0)]
    other = (lax.ppermute(keys, "band", swap), lax.ppermute(values, "band", swap))
    queries = project_queries(normed, spatial_turned, head_count)
    chunks = chunks_of(tokens, peers)
    residuals, gathered = [], []
    for place, (first, size) in enumerate(chunks):
        slots = peers if by_permutes(place, peers) else 0
        residual, *temporal_in = attend(
            first, size, first == 0, slots, frame, hidden, (queries, keys, values), other,
            spatial_out, modulation, placed,
        )
        residuals.append(residual)
        if slots:
            temporal_in = [part[None] for part in temporal_in]
        else:
            temporal_in = [temporal_in[0].reshape(peers, size // peers, -1)]
        gathered.append(exchange(temporal_in, peers))
    last = residuals[-1]
    returned = []
    for parts in gathered:
        mixed = mix_frames(parts, temporal_turned, attended, (last,))
        returned.append(exchange(mixed, peers))
    so_far = ()
    for (first, _), residual, mixed in zip(chunks, residuals, returned):
        mixed = [part.reshape(-1, attended) for part in mixed]
        so_far = finish(
            first, so_far, level_index, time_table, frame, residual, mixed, temporal_out,
            modulation, final_gain[None, :], jnp.transpose(out_weight), latents[0], tokens,
        )
    hidden_out, velocity, update = so_far
    shifted = from_behind(update, "frame", 1).astype(jnp.float32)[None]
    next_latents = jnp.where(lax.axis_index("frame") == 0, fresh_noise[None], shifted)
    return (hidden_out[None], velocity[None], next_latents)


def solution(mesh):
    placed = (
        P(("groups", "frame"), "band", None),
        P(("groups", "frame"), "band", None),
        P(("groups", "band"), None),
        P(("groups", "frame")),
        P(),
        P("groups"),
        P(),
        P(),
        P(),
        P(),
        P(),
        P(),
        P(),
        P(),
    )
    return jax.shard_map(
        steps,
        mesh=mesh,
        in_specs=placed,
        out_specs=(
            P(("groups", "frame"), "band", None),
            P(("groups", "frame"), "band", None),
            P(("groups", "frame"), "band", None),
        ),
        check_vma=False,
    )
```

```python
import functools
import math

import jax
import jax.numpy as jnp
from jax import lax
from jax.experimental import pallas as pl
from jax.experimental.pallas import tpu as pltpu
from jax.sharding import PartitionSpec as P


HEAD_SIZE = 72

VALUE_ROWS = 80
PADDED = 128
LANES = 128
QUERY_BLOCK = 256
KEY_BLOCK = 256

epsilon = 1e-06
scale_of_scores = math.log2(math.e) / math.sqrt(HEAD_SIZE)

WHOLE = pl.BlockSpec(memory_space=pltpu.VMEM)
SCALARS = pl.BlockSpec(memory_space=pltpu.SMEM)
REMAIN = pl.BlockSpec(memory_space=pltpu.HBM)
PARAMS = pltpu.CompilerParams(vmem_limit_bytes=24 * 1024 * 1024)
ACROSS = (((1,), (1,)), ((), ()))


def round_up(value, multiple):
    return (value + multiple - 1) // multiple * multiple


def from_behind(value, axis, steps):
    count = lax.axis_size(axis)
    initial, last = (max(0, -steps), min(count, count - steps))
    return lax.ppermute(value, axis, [(source, source + steps) for source in range(initial, last)])


def normalized(values):
    average = jnp.mean(values, axis=-1, keepdims=True)
    centred = values - average
    variance = jnp.mean(centred * centred, axis=-1, keepdims=True)
    return centred * lax.rsqrt(variance + epsilon)


def padded_rows(rows, total, first_fill):
    columns = rows.shape[1]
    fill = jnp.zeros((total - rows.shape[0], columns), jnp.float32)
    if first_fill:
        fill = jnp.where(lax.broadcasted_iota(jnp.int32, fill.shape, 0) == 0, 1.0, 0.0)
    return jnp.concatenate([rows, fill], axis=0)


def as_query(rows):
    return padded_rows(rows * scale_of_scores, PADDED, False).astype(jnp.bfloat16)


def as_key(rows):
    return jnp.transpose(padded_rows(rows, PADDED, False)).astype(jnp.bfloat16)


def as_value(rows):
    return padded_rows(rows, VALUE_ROWS, True).astype(jnp.bfloat16)


def sinusoid_row(position, width, half, sine_first):
    index = lax.broadcasted_iota(jnp.int32, (1, width), 1)
    place = jnp.where(index < half, index, index - half).astype(jnp.float32)
    angles = position * jnp.exp(-math.log(10000.0) * place / half)
    first, second = (jnp.sin(angles), jnp.cos(angles))
    if not sine_first:
        first, second = (second, first)
    return jnp.where(index < half, first, second)


def cost(microseconds):
    return pl.CostEstimate(
        flops=int(microseconds * 1e9), transcendentals=0, bytes_accessed=1024 * 1024
    )


def in_hbm(*arrays):
    return tuple(pltpu.with_memory_space_constraint(array, pltpu.HBM) for array in arrays)


def start_all(copies):
    for copy in copies:
        copy.start()
    return copies


def keys_values_kernel(
    level, offset, frame, table_far, hidden_far, mod_far, time_far, weight_far,
    keys, values, normed, modulation, placed, delta,
    hidden, time_weight, weight, mod_table, table, sems,
):
    rows_total, width = hidden.shape
    head_count = keys.shape[0]
    attended = head_count * HEAD_SIZE
    table_copy = pltpu.make_async_copy(table_far, table, sems.at[4])
    mod_copy = pltpu.make_async_copy(mod_far, mod_table, sems.at[5])
    start_all([table_copy, mod_copy])
    time_copy = pltpu.make_async_copy(time_far, time_weight, sems.at[0])
    hidden_copy = pltpu.make_async_copy(hidden_far, hidden, sems.at[1])
    weight_copies = [
        pltpu.make_async_copy(
            weight_far.at[pl.ds((1 + part) * attended, attended), :],
            weight.at[pl.ds(part * attended, attended), :],
            sems.at[2 + part],
        )
        for part in range(2)
    ]
    start_all([time_copy, hidden_copy] + weight_copies)
    placed[...] = sinusoid_row(
        (frame[0] + offset[0]).astype(jnp.float32), width, width // 2, True
    )
    table_copy.wait()
    now = table[level[0]].astype(jnp.float32)
    following = table[level[0] - 1].astype(jnp.float32)
    delta[...] = jnp.full(delta.shape, (following - now) / 1000.0, jnp.float32)
    frequencies = time_weight.shape[0]
    embedded = sinusoid_row(now, frequencies, frequencies // 2, False)
    activated = (embedded * (1.0 / (1.0 + jnp.exp(-embedded)))).astype(jnp.bfloat16)
    spread = jnp.broadcast_to(activated.astype(jnp.float32), (16, frequencies)).astype(jnp.bfloat16)
    mod_copy.wait()
    time_copy.wait()
    projected = jnp.dot(spread, time_weight[...], preferred_element_type=jnp.float32)
    lined = jnp.concatenate([mod_table[row : row + 1, :] for row in range(mod_table.shape[0])], axis=1)
    modulation[...] = lined + projected[:1, :]
    shift = modulation[:, :width]
    scale = 1.0 + modulation[:, width : 2 * width]
    hidden_copy.wait()
    for start in range(0, rows_total, QUERY_BLOCK):
        span = slice(start, start + QUERY_BLOCK)
        block = hidden[span, :].astype(jnp.float32)
        normed[span, :] = (normalized(block) * scale + shift).astype(jnp.bfloat16)
        if start == 0:
            weight_copies[0].wait()
            weight_copies[1].wait()
        turned = lax.dot_general(
            weight[...], normed[span, :], ACROSS, preferred_element_type=jnp.float32
        )
        for head in range(head_count):
            first = head * HEAD_SIZE
            keys[head, span, :] = as_key(turned[first : first + HEAD_SIZE, :])
            first += attended
            values[head, :, span] = as_value(turned[first : first + HEAD_SIZE, :])


def keys_and_values(level, table, offset, frame, hidden, mod_table, time_weight, weight, head_count):
    rows, width = hidden.shape
    far = in_hbm(table, hidden, mod_table, time_weight, weight)
    return pl.pallas_call(
        keys_values_kernel,
        out_shape=(
            jax.ShapeDtypeStruct((head_count, rows, PADDED), jnp.bfloat16),
            jax.ShapeDtypeStruct((head_count, VALUE_ROWS, rows), jnp.bfloat16),
            jax.ShapeDtypeStruct((rows, width), jnp.bfloat16),
            jax.ShapeDtypeStruct((1, mod_table.size), jnp.float32),
            jax.ShapeDtypeStruct((1, width), jnp.float32),
            jax.ShapeDtypeStruct((1, LANES), jnp.float32),
        ),
        in_specs=[SCALARS] * 3 + [REMAIN] * 5,
        out_specs=(WHOLE,) * 6,
        scratch_shapes=[
            pltpu.VMEM(hidden.shape, jnp.bfloat16),
            pltpu.VMEM(time_weight.shape, jnp.bfloat16),
            pltpu.VMEM((2 * head_count * HEAD_SIZE, width), jnp.bfloat16),
            pltpu.VMEM(mod_table.shape, jnp.float32),
            pltpu.SMEM(table.shape, jnp.int32),
            pltpu.SemaphoreType.DMA((6,)),
        ],
        compiler_params=PARAMS,
        cost_estimate=cost(5),
        name="keys_and_values",
    )(level, offset, frame, *far)


def queries_kernel(normed, weight_far, queries, weight, sems):
    head_count = queries.shape[0]
    attended = head_count * HEAD_SIZE
    copy = pltpu.make_async_copy(weight_far.at[pl.ds(0, attended), :], weight, sems.at[0])
    copy.start()
    copy.wait()
    for start in range(0, normed.shape[0], QUERY_BLOCK):
        span = slice(start, start + QUERY_BLOCK)
        turned = lax.dot_general(
            weight[...], normed[span, :], ACROSS, preferred_element_type=jnp.float32
        )
        for head in range(head_count):
            first = head * HEAD_SIZE
            queries[head, :, span] = as_query(turned[first : first + HEAD_SIZE, :])


def project_queries(normed, weight, head_count):
    rows, width = normed.shape
    return pl.pallas_call(
        queries_kernel,
        out_shape=jax.ShapeDtypeStruct((head_count, PADDED, rows), jnp.bfloat16),
        in_specs=[WHOLE, REMAIN],
        out_specs=WHOLE,
        scratch_shapes=[
            pltpu.VMEM((head_count * HEAD_SIZE, width), jnp.bfloat16),
            pltpu.SemaphoreType.DMA((1,)),
        ],
        compiler_params=PARAMS,
        cost_estimate=cost(3),
        name="project_queries",
    )(normed, *in_hbm(weight))


def turn_back(turned, rows, attended):
    for start in range(0, attended, LANES):
        rows[:, start : start + LANES] = jnp.transpose(
            turned[start : start + LANES, :]
        ).astype(jnp.bfloat16)


def share_out(total):
    return total[:HEAD_SIZE, :] / total[HEAD_SIZE : HEAD_SIZE + 1, :]


def attend_kernel(
    first, resident, slots,
    frame, hidden_far, queries_in, keys_in, values_in, other_keys_in, other_values_in, weight_far,
    modulation, placed,
    residual_far, *refs,
):
    outs = max(slots, 1)
    temporal_far = refs[:outs]
    scores_a, scores_b, turned, rows, hidden, weight, residual, temporal_in, sems, *loaded = refs[outs:]
    count, width = residual.shape
    head_count = queries_in.shape[0]
    attended = head_count * HEAD_SIZE
    half = keys_in.shape[1]
    near = (queries_in, keys_in, values_in, other_keys_in, other_values_in)
    if not resident:
        far = (queries_in.at[:, :, pl.ds(first, count)],) + near[1:]
        near = loaded

        def head_copies(head):
            return [
                pltpu.make_async_copy(
                    source.at[head], target.at[head], sems.at[2 + head * len(near) + place]
                )
                for place, (source, target) in enumerate(zip(far, near))
            ]

        for head in range(head_count):
            start_all(head_copies(head))
    hidden_copy = pltpu.make_async_copy(
        hidden_far.at[pl.ds(first, count), :], hidden, sems.at[0]
    )
    weight_copy = pltpu.make_async_copy(weight_far, weight, sems.at[1])
    start_all([hidden_copy, weight_copy])
    queries, keys, values, other_keys, other_values = near
    stored = 2 + len(loaded) * head_count
    begin = first if resident else 0
    block = scores_a.shape[1]
    turned[attended:, :] = jnp.zeros((turned.shape[0] - attended, block), jnp.float32)
    stores = []
    for start in range(0, count, block):
        span = slice(begin + start, begin + start + block)
        spots = [
            (side, key, slice(key, key + KEY_BLOCK), slice(side * half + key, side * half + key + KEY_BLOCK))
            for side in range(2)
            for key in range(0, half, KEY_BLOCK)
        ]

        def arrive(head):
            if start == 0 and not resident:
                for copy in head_copies(head):
                    copy.wait()

        def advance(scored, scores, mixed, known, top):
            highest, total = (None, None)
            for side, _, local, place in spots:
                if scored is not None:
                    part = jnp.dot(
                        (keys, other_keys)[side][scored, local, :], queries[scored, :, span],
                        preferred_element_type=jnp.float32,
                    )
                    scores[place, :] = part
                    peak = jnp.max(part, axis=0, keepdims=True)
                    highest = peak if highest is None else jnp.maximum(highest, peak)
                if mixed is not None:
                    weights = jnp.exp2(known[place, :] - top).astype(jnp.bfloat16)
                    part = jnp.dot(
                        (values, other_values)[side][mixed, :, local], weights,
                        preferred_element_type=jnp.float32,
                    )
                    total = part if total is None else total + part
            if mixed is not None:
                begin_row = mixed * HEAD_SIZE
                if not isinstance(mixed, int):
                    begin_row = pl.multiple_of(begin_row, 8)
                turned[pl.ds(begin_row, HEAD_SIZE), :] = share_out(total)
            return highest

        def pair(index, top):
            arrive(2 * index + 1)
            middle = advance(2 * index + 1, scores_b, 2 * index, scores_a, top)
            arrive(2 * index + 2)
            return advance(2 * index + 2, scores_a, 2 * index + 1, scores_b, middle)

        arrive(0)
        top = lax.fori_loop(
            0, head_count // 2 - 1, pair, advance(0, scores_a, None, None, None)
        )
        arrive(head_count - 1)
        top = advance(head_count - 1, scores_b, head_count - 2, scores_a, top)
        advance(None, None, head_count - 1, scores_b, top)
        turn_back(turned, rows, attended)
        if start == 0:
            hidden_copy.wait()
            weight_copy.wait()
        gate = modulation[:, 2 * width :]
        step = QUERY_BLOCK // 2
        for part in range(0, block, step):
            span = slice(start + part, start + part + step)
            term = jnp.dot(
                rows[part : part + step, :attended], weight[...],
                preferred_element_type=jnp.float32,
            )
            kept = hidden[span, :].astype(jnp.float32) + gate * term
            residual[span, :] = kept
            temporal_in[span, :] = (kept + placed[...]).astype(jnp.bfloat16)
            window = pl.ds(start + part, step)
            moves = [(residual.at[window, :], residual_far.at[window, :])]
            if not slots:
                moves.append((temporal_in.at[window, :], temporal_far[0].at[window, :]))
            stores += start_all(
                [
                    pltpu.make_async_copy(source, target, sems.at[stored + len(stores) + place])
                    for place, (source, target) in enumerate(moves)
                ]
            )
    share = count // outs
    for slot in range(slots):
        window = pl.ds(pl.multiple_of(lax.bitwise_xor(frame[0], slot) * share, 16), share)
        copy = pltpu.make_async_copy(
            temporal_in.at[window, :], temporal_far[slot], sems.at[stored + len(stores)]
        )
        copy.start()
        stores.append(copy)
    for copy in stores:
        copy.wait()


def attend(first, count, resident, slots, frame, hidden, projected, other, out_weight, modulation, placed):
    queries, keys, values = projected
    head_count = queries.shape[0]
    width = hidden.shape[1]
    attended = out_weight.shape[0]
    deep = round_up(attended, LANES)
    near = WHOLE if resident else REMAIN
    loaded = ()
    hidden, out_weight = in_hbm(hidden, out_weight)
    if not resident:
        queries, keys, values, *other = in_hbm(queries, keys, values, *other)
        loaded = tuple(
            pltpu.VMEM(shape, jnp.bfloat16)
            for shape in ((head_count, PADDED, count), keys.shape, values.shape, keys.shape, values.shape)
        )
    sem_count = 2 + len(loaded) * head_count + 4 * (count // QUERY_BLOCK) + slots
    outs = max(slots, 1)
    block = 2 * QUERY_BLOCK if count % (2 * QUERY_BLOCK) == 0 else QUERY_BLOCK
    return pl.pallas_call(
        functools.partial(attend_kernel, first, resident, slots),
        out_shape=(
            pltpu.HBM((count, width), jnp.float32),
            *[pltpu.HBM((count // outs, width), jnp.bfloat16)] * outs,
        ),
        in_specs=[SCALARS, REMAIN] + [near] * 5 + [REMAIN] + [WHOLE] * 2,
        out_specs=(REMAIN,) * (1 + outs),
        scratch_shapes=[
            pltpu.VMEM((2 * keys.shape[1], block), jnp.float32),
            pltpu.VMEM((2 * keys.shape[1], block), jnp.float32),
            pltpu.VMEM((deep, block), jnp.float32),
            pltpu.VMEM((block, deep), jnp.bfloat16),
            pltpu.VMEM((count, width), jnp.bfloat16),
            pltpu.VMEM(out_weight.shape, jnp.bfloat16),
            pltpu.VMEM((count, width), jnp.float32),
            pltpu.VMEM((count, width), jnp.bfloat16),
            pltpu.SemaphoreType.DMA((sem_count,)),
            *loaded,
        ],
        compiler_params=PARAMS,
        cost_estimate=cost(0.028 * count),
        name="attend",
    )(frame, hidden, queries, keys, values, *other, out_weight, modulation, placed)


def temporal_kernel(group, tokens, parts, frame, *refs):
    gathered, weight_far, mixed = (refs[:parts], refs[parts], refs[-8])
    weight, turned, bias, scores, turned_out, rows, sems = refs[-7:]
    frames, share, width = gathered[0].shape
    attended = mixed.shape[2]
    head_count = attended // HEAD_SIZE
    count = bias.shape[0]
    pieces = sems.shape[0]
    height = weight.shape[0] // pieces
    weight_copies = start_all(
        [
            pltpu.make_async_copy(
                weight_far.at[pl.ds(piece * height, height), :],
                weight.at[pl.ds(piece * height, height), :],
                sems.at[piece],
            )
            for piece in range(pieces)
        ]
    )
    own = lax.rem(lax.broadcasted_iota(jnp.int32, (count, count), 0), tokens)
    other = lax.rem(lax.broadcasted_iota(jnp.int32, (count, count), 1), tokens)
    bias[...] = jnp.where(own == other, 0.0, -1e30)
    turned_out[attended:, :] = jnp.zeros((turned_out.shape[0] - attended, count), jnp.float32)
    for start in range(0, share, group):
        block = jnp.concatenate(
            [part[:, start : start + group, :].reshape(frames * group, width) for part in gathered],
            axis=0,
        )
        for piece in range(pieces):
            if start == 0:
                weight_copies[piece].wait()
            span = slice(piece * height, (piece + 1) * height)
            turned[span, :] = lax.dot_general(
                weight[span, :], block, ACROSS, preferred_element_type=jnp.float32
            )
        together = scores.shape[0]
        for begin in range(0, head_count, together):
            tops = []
            for place in range(together):
                first = (begin + place) * HEAD_SIZE
                query = turned[first : first + HEAD_SIZE, :]
                key = turned[attended + first : attended + first + HEAD_SIZE, :]
                found = jnp.dot(as_key(key), as_query(query), preferred_element_type=jnp.float32)
                found = found + bias[...]
                scores[place, :, :] = found
                tops.append(jnp.max(found, axis=0, keepdims=True))
            for place in range(together):
                first = (begin + place) * HEAD_SIZE
                value = turned[2 * attended + first : 2 * attended + first + HEAD_SIZE, :]
                weights = jnp.exp2(scores[place, :, :] - tops[place]).astype(jnp.bfloat16)
                total = jnp.dot(as_value(value), weights, preferred_element_type=jnp.float32)
                turned_out[first : first + HEAD_SIZE, :] = share_out(total)
        turn_back(turned_out, rows, attended)
        for slot in range(parts):
            span = slice(slot * frames * group, (slot + 1) * frames * group)
            owner = lax.bitwise_xor(frame[0], slot) if parts > 1 else 0
            mixed[pl.ds(owner, frames), start : start + group, :] = rows[span, :attended].reshape(
                frames, group, attended
            )


def mix_frames(frame, gathered, weight, attended, after):
    parts = len(gathered)
    given = gathered[0].shape
    frames, share, width = given
    whole = parts * frames
    group = QUERY_BLOCK // whole if QUERY_BLOCK % whole == 0 else 0
    shape, tokens = given, group
    if group == 0 or group % 16 or share % group:
        shape, group, tokens = ((1, frames * share, width), frames * share, share)
    count = parts * shape[0] * group
    together = attended // HEAD_SIZE if count <= QUERY_BLOCK else 1
    deep = round_up(attended, LANES)
    mixed = pl.pallas_call(
        functools.partial(temporal_kernel, group, tokens, parts),
        out_shape=jax.ShapeDtypeStruct((parts * shape[0], shape[1], attended), jnp.bfloat16),
        in_specs=[SCALARS] + [WHOLE] * parts + [REMAIN] * (1 + len(after)),
        out_specs=WHOLE,
        scratch_shapes=[
            pltpu.VMEM(weight.shape, jnp.bfloat16),
            pltpu.VMEM((weight.shape[0], count), jnp.float32),
            pltpu.VMEM((count, count), jnp.float32),
            pltpu.VMEM((together, count, count), jnp.float32),
            pltpu.VMEM((deep, count), jnp.float32),
            pltpu.VMEM((count, deep), jnp.bfloat16),
            pltpu.SemaphoreType.DMA((9,)),
        ],
        compiler_params=PARAMS,
        cost_estimate=cost(0.025 * count),
        name="mix_frames",
    )(frame, *[part.reshape(shape) for part in gathered], *in_hbm(weight, *after))
    return mixed.reshape(whole, share, attended)


def finish_kernel(
    first, delta, residual_far, mixed, weight, modulation, gain, out_weight, latents, *refs,
):
    hidden_far, velocity_far, update_far, residual, hidden, velocity, update, sems = refs[-8:]
    blocks = residual.shape[0] // QUERY_BLOCK
    loads = start_all(
        [
            pltpu.make_async_copy(
                residual_far.at[pl.ds(block * QUERY_BLOCK, QUERY_BLOCK), :],
                residual.at[pl.ds(block * QUERY_BLOCK, QUERY_BLOCK), :],
                sems.at[2 + blocks + block],
            )
            for block in range(blocks)
        ]
    )
    count, width = residual.shape
    channels = out_weight.shape[0]
    fold = LANES // channels
    lines = pl.ds(first // fold, count // fold)
    spread = lax.rem(lax.broadcasted_iota(jnp.int32, (LANES, channels), 0), channels)
    spread = jnp.where(
        spread == lax.broadcasted_iota(jnp.int32, (LANES, channels), 1), 1.0, 0.0
    ).astype(jnp.bfloat16)
    repeated = jnp.dot(spread, out_weight[...], preferred_element_type=jnp.float32)
    repeated = repeated.astype(jnp.bfloat16)
    stores = []
    for start in range(0, count, QUERY_BLOCK):
        span = slice(start, start + QUERY_BLOCK)
        term = jnp.dot(mixed[span, :], weight[...], preferred_element_type=jnp.float32)
        loads[start // QUERY_BLOCK].wait()
        block = residual[span, :] + modulation[:, 2 * width :] * term
        hidden[span, :] = block.astype(jnp.bfloat16)
        copy = pltpu.make_async_copy(
            hidden.at[pl.ds(start, QUERY_BLOCK), :],
            hidden_far.at[pl.ds(first + start, QUERY_BLOCK), :],
            sems.at[2 + len(stores)],
        )
        copy.start()
        stores.append(copy)
        final_rows = (normalized(block) * gain[...]).astype(jnp.bfloat16)
        wide = lax.dot_general(final_rows, repeated, ACROSS, preferred_element_type=jnp.float32)
        row = lax.rem(lax.broadcasted_iota(jnp.int32, (QUERY_BLOCK, LANES), 0), fold)
        lane = lax.broadcasted_iota(jnp.int32, (QUERY_BLOCK, LANES), 1) // channels
        picked = jnp.where(row == lane, wide, 0.0).reshape(QUERY_BLOCK // fold, fold, LANES)
        velocity[start // fold : (start + QUERY_BLOCK) // fold, :] = jnp.sum(picked, axis=1)
    known = latents[first // fold : (first + count) // fold, :]
    update[...] = (known + delta[...] * velocity[...]).astype(jnp.bfloat16)
    stores += start_all(
        [
            pltpu.make_async_copy(velocity, velocity_far.at[lines, :], sems.at[0]),
            pltpu.make_async_copy(update, update_far.at[lines, :], sems.at[1]),
        ]
    )
    for copy in stores:
        copy.wait()


def finish(first, so_far, delta, residual, mixed, weight, modulation, gain, out_weight, latents, tokens):
    count, width = residual.shape
    lines = count * out_weight.shape[0] // LANES
    known = 8
    (residual,) = in_hbm(residual)
    return pl.pallas_call(
        functools.partial(finish_kernel, first),
        out_shape=(
            pltpu.HBM((tokens, width), jnp.bfloat16),
            pltpu.HBM(latents.shape, jnp.float32),
            pltpu.HBM(latents.shape, jnp.bfloat16),
        ),
        in_specs=[WHOLE, REMAIN] + [WHOLE] * 6 + [REMAIN] * len(so_far),
        out_specs=(REMAIN,) * 3,
        scratch_shapes=[
            pltpu.VMEM((count, width), jnp.float32),
            pltpu.VMEM((count, width), jnp.bfloat16),
            pltpu.VMEM((lines, LANES), jnp.float32),
            pltpu.VMEM((lines, LANES), jnp.bfloat16),
            pltpu.SemaphoreType.DMA((2 + 2 * (count // QUERY_BLOCK),)),
        ],
        input_output_aliases={known + place: place for place in range(len(so_far))},
        compiler_params=PARAMS,
        cost_estimate=cost(0.012 * count),
        name="finish",
    )(delta, residual, mixed, weight, modulation, gain, out_weight, latents, *so_far)


FIRST_BLOCKS = 1
PERMUTED = (1,)


def chunks_of(tokens, peers):
    least = round_up(QUERY_BLOCK, 16 * peers)
    head = FIRST_BLOCKS * least
    if least % QUERY_BLOCK or tokens % least or head >= tokens:
        return [(0, tokens)]
    return [(0, head), (head, tokens - head)]


def by_permutes(place, peers):
    return place in PERMUTED and peers & (peers - 1) == 0


def exchange(parts, peers):
    if len(parts) == 1:
        return [lax.all_to_all(parts[0], "frame", 0, 0, tiled=True)]
    arrived = [parts[0]]
    for slot in range(1, peers):
        pairs = [(index, index ^ slot) for index in range(peers)]
        arrived.append(lax.ppermute(parts[slot], "frame", pairs))
    return arrived


def steps(
    hidden_in,
    latents,
    fresh_noise,
    level_index,
    time_table,
    frame_offset,
    mod_table,
    time_weight,
    spatial_qkv,
    spatial_out,
    temporal_qkv,
    temporal_out,
    final_gain,
    out_weight,
):
    tokens = hidden_in.shape[1]
    attended = spatial_out.shape[0]
    head_count = attended // HEAD_SIZE
    peers = lax.axis_size("frame")
    hidden = hidden_in[0]
    frame = lax.axis_index("frame").astype(jnp.int32).reshape(1)
    spatial_turned = jnp.transpose(spatial_qkv)
    temporal_turned = jnp.transpose(temporal_qkv)
    keys, values, normed, modulation, placed, delta = keys_and_values(
        level_index, time_table, frame_offset, frame, hidden, mod_table.reshape(-1, LANES),
        time_weight, spatial_turned, head_count,
    )
    swap = [(0, 1), (1, 0)]
    other = (lax.ppermute(keys, "band", swap), lax.ppermute(values, "band", swap))
    queries = project_queries(normed, spatial_turned, head_count)
    chunks = chunks_of(tokens, peers)
    residuals, gathered = [], []
    for place, (first, size) in enumerate(chunks):
        slots = peers if by_permutes(place, peers) else 0
        residual, *temporal_in = attend(
            first, size, first == 0, slots, frame, hidden, (queries, keys, values), other,
            spatial_out, modulation, placed,
        )
        residuals.append(residual)
        if slots:
            temporal_in = [part[None] for part in temporal_in]
        else:
            temporal_in = [temporal_in[0].reshape(peers, size // peers, -1)]
        gathered.append(exchange(temporal_in, peers))
    last = residuals[-1]
    returned = []
    for parts in gathered:
        mixed = mix_frames(frame, parts, temporal_turned, attended, (last,))
        returned.append(exchange([mixed], peers)[0])
    so_far = ()
    for (first, _), residual, mixed in zip(chunks, residuals, returned):
        so_far = finish(
            first, so_far, delta, residual, mixed.reshape(-1, attended), temporal_out,
            modulation, final_gain[None, :], jnp.transpose(out_weight), latents[0], tokens,
        )
    hidden_out, velocity, update = so_far
    shifted = from_behind(update, "frame", 1).astype(jnp.float32)[None]
    next_latents = jnp.where(lax.axis_index("frame") == 0, fresh_noise[None], shifted)
    return (hidden_out[None], velocity[None], next_latents)


def solution(mesh):
    placed = (
        P(("groups", "frame"), "band", None),
        P(("groups", "frame"), "band", None),
        P(("groups", "band"), None),
        P(("groups", "frame")),
        P(),
        P("groups"),
        P(),
        P(),
        P(),
        P(),
        P(),
        P(),
        P(),
        P(),
    )
    return jax.shard_map(
        steps,
        mesh=mesh,
        in_specs=placed,
        out_specs=(
            P(("groups", "frame"), "band", None),
            P(("groups", "frame"), "band", None),
            P(("groups", "frame"), "band", None),
        ),
        check_vma=False,
    )
```

```python
import functools
import math

import jax
import jax.numpy as jnp
from jax import lax
from jax.experimental import pallas as pl
from jax.experimental.pallas import tpu as pltpu
from jax.sharding import PartitionSpec as P


HEAD_SIZE = 72

VALUE_ROWS = 80
PADDED = 128
LANES = 128
QUERY_BLOCK = 256
KEY_BLOCK = 256

epsilon = 1e-06
scale_of_scores = math.log2(math.e) / math.sqrt(HEAD_SIZE)

WHOLE = pl.BlockSpec(memory_space=pltpu.VMEM)
SCALARS = pl.BlockSpec(memory_space=pltpu.SMEM)
REMAIN = pl.BlockSpec(memory_space=pltpu.HBM)
PARAMS = pltpu.CompilerParams(vmem_limit_bytes=24 * 1024 * 1024)
ACROSS = (((1,), (1,)), ((), ()))


def round_up(value, multiple):
    return (value + multiple - 1) // multiple * multiple


def from_behind(value, axis, steps):
    count = lax.axis_size(axis)
    initial, last = (max(0, -steps), min(count, count - steps))
    return lax.ppermute(value, axis, [(source, source + steps) for source in range(initial, last)])


def normalized(values):
    average = jnp.mean(values, axis=-1, keepdims=True)
    centred = values - average
    variance = jnp.mean(centred * centred, axis=-1, keepdims=True)
    return centred * lax.rsqrt(variance + epsilon)


def padded_rows(rows, total, first_fill):
    columns = rows.shape[1]
    fill = jnp.zeros((total - rows.shape[0], columns), jnp.float32)
    if first_fill:
        fill = jnp.where(lax.broadcasted_iota(jnp.int32, fill.shape, 0) == 0, 1.0, 0.0)
    return jnp.concatenate([rows, fill], axis=0)


def as_query(rows):
    return padded_rows(rows * scale_of_scores, PADDED, False).astype(jnp.bfloat16)


def as_key(rows):
    return jnp.transpose(padded_rows(rows, PADDED, False)).astype(jnp.bfloat16)


def as_value(rows):
    return padded_rows(rows, VALUE_ROWS, True).astype(jnp.bfloat16)


def sinusoid_row(position, width, half, sine_first):
    index = lax.broadcasted_iota(jnp.int32, (1, width), 1)
    place = jnp.where(index < half, index, index - half).astype(jnp.float32)
    angles = position * jnp.exp(-math.log(10000.0) * place / half)
    first, second = (jnp.sin(angles), jnp.cos(angles))
    if not sine_first:
        first, second = (second, first)
    return jnp.where(index < half, first, second)


def cost(microseconds):
    return pl.CostEstimate(
        flops=int(microseconds * 1e9), transcendentals=0, bytes_accessed=1024 * 1024
    )


def in_hbm(*arrays):
    return tuple(pltpu.with_memory_space_constraint(array, pltpu.HBM) for array in arrays)


def start_all(copies):
    for copy in copies:
        copy.start()
    return copies


def keys_values_kernel(
    level, offset, frame, table_far, hidden_far, mod_far, time_far, weight_far,
    keys, values, normed, modulation, placed, delta,
    hidden, time_weight, weight, mod_table, table, sems,
):
    rows_total, width = hidden.shape
    head_count = keys.shape[0]
    attended = head_count * HEAD_SIZE
    table_copy = pltpu.make_async_copy(table_far, table, sems.at[4])
    mod_copy = pltpu.make_async_copy(mod_far, mod_table, sems.at[5])
    start_all([table_copy, mod_copy])
    time_copy = pltpu.make_async_copy(time_far, time_weight, sems.at[0])
    hidden_copy = pltpu.make_async_copy(hidden_far, hidden, sems.at[1])
    weight_copies = [
        pltpu.make_async_copy(
            weight_far.at[pl.ds((1 + part) * attended, attended), :],
            weight.at[pl.ds(part * attended, attended), :],
            sems.at[2 + part],
        )
        for part in range(2)
    ]
    start_all([time_copy, hidden_copy] + weight_copies)
    placed[...] = sinusoid_row(
        (frame[0] + offset[0]).astype(jnp.float32), width, width // 2, True
    )
    table_copy.wait()
    now = table[level[0]].astype(jnp.float32)
    following = table[level[0] - 1].astype(jnp.float32)
    delta[...] = jnp.full(delta.shape, (following - now) / 1000.0, jnp.float32)
    frequencies = time_weight.shape[0]
    embedded = sinusoid_row(now, frequencies, frequencies // 2, False)
    activated = (embedded * (1.0 / (1.0 + jnp.exp(-embedded)))).astype(jnp.bfloat16)
    spread = jnp.broadcast_to(activated.astype(jnp.float32), (16, frequencies)).astype(jnp.bfloat16)
    mod_copy.wait()
    time_copy.wait()
    projected = jnp.dot(spread, time_weight[...], preferred_element_type=jnp.float32)
    lined = jnp.concatenate([mod_table[row : row + 1, :] for row in range(mod_table.shape[0])], axis=1)
    modulation[...] = lined + projected[:1, :]
    shift = modulation[:, :width]
    scale = 1.0 + modulation[:, width : 2 * width]
    hidden_copy.wait()
    for start in range(0, rows_total, QUERY_BLOCK):
        span = slice(start, start + QUERY_BLOCK)
        block = hidden[span, :].astype(jnp.float32)
        normed[span, :] = (normalized(block) * scale + shift).astype(jnp.bfloat16)
        if start == 0:
            weight_copies[0].wait()
            weight_copies[1].wait()
        turned = lax.dot_general(
            weight[...], normed[span, :], ACROSS, preferred_element_type=jnp.float32
        )
        for head in range(head_count):
            first = head * HEAD_SIZE
            keys[head, span, :] = as_key(turned[first : first + HEAD_SIZE, :])
            first += attended
            values[head, :, span] = as_value(turned[first : first + HEAD_SIZE, :])


def keys_and_values(level, table, offset, frame, hidden, mod_table, time_weight, weight, head_count):
    rows, width = hidden.shape
    far = in_hbm(table, hidden, mod_table, time_weight, weight)
    return pl.pallas_call(
        keys_values_kernel,
        out_shape=(
            jax.ShapeDtypeStruct((head_count, rows, PADDED), jnp.bfloat16),
            jax.ShapeDtypeStruct((head_count, VALUE_ROWS, rows), jnp.bfloat16),
            jax.ShapeDtypeStruct((rows, width), jnp.bfloat16),
            jax.ShapeDtypeStruct((1, mod_table.size), jnp.float32),
            jax.ShapeDtypeStruct((1, width), jnp.float32),
            jax.ShapeDtypeStruct((1, LANES), jnp.float32),
        ),
        in_specs=[SCALARS] * 3 + [REMAIN] * 5,
        out_specs=(WHOLE,) * 6,
        scratch_shapes=[
            pltpu.VMEM(hidden.shape, jnp.bfloat16),
            pltpu.VMEM(time_weight.shape, jnp.bfloat16),
            pltpu.VMEM((2 * head_count * HEAD_SIZE, width), jnp.bfloat16),
            pltpu.VMEM(mod_table.shape, jnp.float32),
            pltpu.SMEM(table.shape, jnp.int32),
            pltpu.SemaphoreType.DMA((6,)),
        ],
        compiler_params=PARAMS,
        cost_estimate=cost(5),
        name="keys_and_values",
    )(level, offset, frame, *far)


def queries_kernel(normed, weight_far, queries, weight, sems):
    head_count = queries.shape[0]
    attended = head_count * HEAD_SIZE
    copy = pltpu.make_async_copy(weight_far.at[pl.ds(0, attended), :], weight, sems.at[0])
    copy.start()
    copy.wait()
    for start in range(0, normed.shape[0], QUERY_BLOCK):
        span = slice(start, start + QUERY_BLOCK)
        turned = lax.dot_general(
            weight[...], normed[span, :], ACROSS, preferred_element_type=jnp.float32
        )
        for head in range(head_count):
            first = head * HEAD_SIZE
            queries[head, :, span] = as_query(turned[first : first + HEAD_SIZE, :])


def project_queries(normed, weight, head_count):
    rows, width = normed.shape
    return pl.pallas_call(
        queries_kernel,
        out_shape=jax.ShapeDtypeStruct((head_count, PADDED, rows), jnp.bfloat16),
        in_specs=[WHOLE, REMAIN],
        out_specs=WHOLE,
        scratch_shapes=[
            pltpu.VMEM((head_count * HEAD_SIZE, width), jnp.bfloat16),
            pltpu.SemaphoreType.DMA((1,)),
        ],
        compiler_params=PARAMS,
        cost_estimate=cost(3),
        name="project_queries",
    )(normed, *in_hbm(weight))


def turn_back(turned, rows, attended):
    for start in range(0, attended, LANES):
        rows[:, start : start + LANES] = jnp.transpose(
            turned[start : start + LANES, :]
        ).astype(jnp.bfloat16)


def share_out(total):
    return total[:HEAD_SIZE, :] / total[HEAD_SIZE : HEAD_SIZE + 1, :]


def attend_kernel(
    first, resident, slots,
    frame, hidden_far, queries_in, keys_in, values_in, other_keys_in, other_values_in, weight_far,
    modulation, placed,
    residual_far, *refs,
):
    outs = max(slots, 1)
    temporal_far = refs[:outs]
    scores_a, scores_b, turned, rows, hidden, weight, residual, temporal_in, sems, *loaded = refs[outs:]
    count, width = residual.shape
    head_count = queries_in.shape[0]
    attended = head_count * HEAD_SIZE
    half = keys_in.shape[1]
    near = (queries_in, keys_in, values_in, other_keys_in, other_values_in)
    if not resident:
        far = (queries_in.at[:, :, pl.ds(first, count)],) + near[1:]
        near = loaded

        def head_copies(head):
            return [
                pltpu.make_async_copy(
                    source.at[head], target.at[head], sems.at[2 + head * len(near) + place]
                )
                for place, (source, target) in enumerate(zip(far, near))
            ]

        for head in range(head_count):
            start_all(head_copies(head))
    hidden_copy = pltpu.make_async_copy(
        hidden_far.at[pl.ds(first, count), :], hidden, sems.at[0]
    )
    weight_copy = pltpu.make_async_copy(weight_far, weight, sems.at[1])
    start_all([hidden_copy, weight_copy])
    queries, keys, values, other_keys, other_values = near
    stored = 2 + len(loaded) * head_count
    begin = first if resident else 0
    block = scores_a.shape[1]
    turned[attended:, :] = jnp.zeros((turned.shape[0] - attended, block), jnp.float32)
    stores = []
    for start in range(0, count, block):
        span = slice(begin + start, begin + start + block)
        spots = [
            (side, key, slice(key, key + KEY_BLOCK), slice(side * half + key, side * half + key + KEY_BLOCK))
            for side in range(2)
            for key in range(0, half, KEY_BLOCK)
        ]

        def arrive(head):
            if start == 0 and not resident:
                for copy in head_copies(head):
                    copy.wait()

        def advance(scored, scores, mixed, known, top):
            highest, total = (None, None)
            for side, _, local, place in spots:
                if scored is not None:
                    part = jnp.dot(
                        (keys, other_keys)[side][scored, local, :], queries[scored, :, span],
                        preferred_element_type=jnp.float32,
                    )
                    scores[place, :] = part
                    peak = jnp.max(part, axis=0, keepdims=True)
                    highest = peak if highest is None else jnp.maximum(highest, peak)
                if mixed is not None:
                    weights = jnp.exp2(known[place, :] - top).astype(jnp.bfloat16)
                    part = jnp.dot(
                        (values, other_values)[side][mixed, :, local], weights,
                        preferred_element_type=jnp.float32,
                    )
                    total = part if total is None else total + part
            if mixed is not None:
                begin_row = mixed * HEAD_SIZE
                if not isinstance(mixed, int):
                    begin_row = pl.multiple_of(begin_row, 8)
                turned[pl.ds(begin_row, HEAD_SIZE), :] = share_out(total)
            return highest

        def pair(index, top):
            arrive(2 * index + 1)
            middle = advance(2 * index + 1, scores_b, 2 * index, scores_a, top)
            arrive(2 * index + 2)
            return advance(2 * index + 2, scores_a, 2 * index + 1, scores_b, middle)

        arrive(0)
        top = lax.fori_loop(
            0, head_count // 2 - 1, pair, advance(0, scores_a, None, None, None)
        )
        arrive(head_count - 1)
        top = advance(head_count - 1, scores_b, head_count - 2, scores_a, top)
        advance(None, None, head_count - 1, scores_b, top)
        turn_back(turned, rows, attended)
        if start == 0:
            hidden_copy.wait()
            weight_copy.wait()
        gate = modulation[:, 2 * width :]
        step = QUERY_BLOCK // 2
        for part in range(0, block, step):
            span = slice(start + part, start + part + step)
            term = jnp.dot(
                rows[part : part + step, :attended], weight[...],
                preferred_element_type=jnp.float32,
            )
            kept = hidden[span, :].astype(jnp.float32) + gate * term
            residual[span, :] = kept
            temporal_in[span, :] = (kept + placed[...]).astype(jnp.bfloat16)
            window = pl.ds(start + part, step)
            moves = [(residual.at[window, :], residual_far.at[window, :])]
            if not slots:
                moves.append((temporal_in.at[window, :], temporal_far[0].at[window, :]))
            stores += start_all(
                [
                    pltpu.make_async_copy(source, target, sems.at[stored + len(stores) + place])
                    for place, (source, target) in enumerate(moves)
                ]
            )
    share = count // outs
    for slot in range(slots):
        window = pl.ds(pl.multiple_of(lax.bitwise_xor(frame[0], slot) * share, 16), share)
        copy = pltpu.make_async_copy(
            temporal_in.at[window, :], temporal_far[slot], sems.at[stored + len(stores)]
        )
        copy.start()
        stores.append(copy)
    for copy in stores:
        copy.wait()


def attend(first, count, resident, slots, frame, hidden, projected, other, out_weight, modulation, placed):
    queries, keys, values = projected
    head_count = queries.shape[0]
    width = hidden.shape[1]
    attended = out_weight.shape[0]
    deep = round_up(attended, LANES)
    near = WHOLE if resident else REMAIN
    loaded = ()
    hidden, out_weight = in_hbm(hidden, out_weight)
    if not resident:
        queries, keys, values, *other = in_hbm(queries, keys, values, *other)
        loaded = tuple(
            pltpu.VMEM(shape, jnp.bfloat16)
            for shape in ((head_count, PADDED, count), keys.shape, values.shape, keys.shape, values.shape)
        )
    sem_count = 2 + len(loaded) * head_count + 4 * (count // QUERY_BLOCK) + slots
    outs = max(slots, 1)
    block = 2 * QUERY_BLOCK if count % (2 * QUERY_BLOCK) == 0 else QUERY_BLOCK
    return pl.pallas_call(
        functools.partial(attend_kernel, first, resident, slots),
        out_shape=(
            pltpu.HBM((count, width), jnp.float32),
            *[pltpu.HBM((count // outs, width), jnp.bfloat16)] * outs,
        ),
        in_specs=[SCALARS, REMAIN] + [near] * 5 + [REMAIN] + [WHOLE] * 2,
        out_specs=(REMAIN,) * (1 + outs),
        scratch_shapes=[
            pltpu.VMEM((2 * keys.shape[1], block), jnp.float32),
            pltpu.VMEM((2 * keys.shape[1], block), jnp.float32),
            pltpu.VMEM((deep, block), jnp.float32),
            pltpu.VMEM((block, deep), jnp.bfloat16),
            pltpu.VMEM((count, width), jnp.bfloat16),
            pltpu.VMEM(out_weight.shape, jnp.bfloat16),
            pltpu.VMEM((count, width), jnp.float32),
            pltpu.VMEM((count, width), jnp.bfloat16),
            pltpu.SemaphoreType.DMA((sem_count,)),
            *loaded,
        ],
        compiler_params=PARAMS,
        cost_estimate=cost(0.028 * count),
        name="attend",
    )(frame, hidden, queries, keys, values, *other, out_weight, modulation, placed)


def temporal_kernel(group, tokens, parts, frame, *refs):
    gathered, weight_far, mixed = (refs[:parts], refs[parts], refs[-8])
    weight, turned, bias, scores, turned_out, rows, sems = refs[-7:]
    frames, share, width = gathered[0].shape
    attended = mixed.shape[2]
    head_count = attended // HEAD_SIZE
    count = bias.shape[0]
    pieces = sems.shape[0]
    height = weight.shape[0] // pieces
    weight_copies = start_all(
        [
            pltpu.make_async_copy(
                weight_far.at[pl.ds(piece * height, height), :],
                weight.at[pl.ds(piece * height, height), :],
                sems.at[piece],
            )
            for piece in range(pieces)
        ]
    )
    own = lax.rem(lax.broadcasted_iota(jnp.int32, (count, count), 0), tokens)
    other = lax.rem(lax.broadcasted_iota(jnp.int32, (count, count), 1), tokens)
    bias[...] = jnp.where(own == other, 0.0, -1e30)
    turned_out[attended:, :] = jnp.zeros((turned_out.shape[0] - attended, count), jnp.float32)
    for start in range(0, share, group):
        block = jnp.concatenate(
            [part[:, start : start + group, :].reshape(frames * group, width) for part in gathered],
            axis=0,
        )
        for piece in range(pieces):
            if start == 0:
                weight_copies[piece].wait()
            span = slice(piece * height, (piece + 1) * height)
            turned[span, :] = lax.dot_general(
                weight[span, :], block, ACROSS, preferred_element_type=jnp.float32
            )
        together = scores.shape[0]
        for begin in range(0, head_count, together):
            tops = []
            for place in range(together):
                first = (begin + place) * HEAD_SIZE
                query = turned[first : first + HEAD_SIZE, :]
                key = turned[attended + first : attended + first + HEAD_SIZE, :]
                found = jnp.dot(as_key(key), as_query(query), preferred_element_type=jnp.float32)
                found = found + bias[...]
                scores[place, :, :] = found
                tops.append(jnp.max(found, axis=0, keepdims=True))
            for place in range(together):
                first = (begin + place) * HEAD_SIZE
                value = turned[2 * attended + first : 2 * attended + first + HEAD_SIZE, :]
                weights = jnp.exp2(scores[place, :, :] - tops[place]).astype(jnp.bfloat16)
                total = jnp.dot(as_value(value), weights, preferred_element_type=jnp.float32)
                turned_out[first : first + HEAD_SIZE, :] = share_out(total)
        turn_back(turned_out, rows, attended)
        for slot in range(parts):
            span = slice(slot * frames * group, (slot + 1) * frames * group)
            owner = lax.bitwise_xor(frame[0], slot) if parts > 1 else 0
            mixed[pl.ds(owner, frames), start : start + group, :] = rows[span, :attended].reshape(
                frames, group, attended
            )


def mix_frames(frame, gathered, weight, attended, after):
    parts = len(gathered)
    given = gathered[0].shape
    frames, share, width = given
    whole = parts * frames
    group = QUERY_BLOCK // whole if QUERY_BLOCK % whole == 0 else 0
    shape, tokens = given, group
    if group == 0 or group % 16 or share % group:
        shape, group, tokens = ((1, frames * share, width), frames * share, share)
    count = parts * shape[0] * group
    together = attended // HEAD_SIZE if count <= QUERY_BLOCK else 1
    deep = round_up(attended, LANES)
    mixed = pl.pallas_call(
        functools.partial(temporal_kernel, group, tokens, parts),
        out_shape=jax.ShapeDtypeStruct((parts * shape[0], shape[1], attended), jnp.bfloat16),
        in_specs=[SCALARS] + [WHOLE] * parts + [REMAIN] * (1 + len(after)),
        out_specs=WHOLE,
        scratch_shapes=[
            pltpu.VMEM(weight.shape, jnp.bfloat16),
            pltpu.VMEM((weight.shape[0], count), jnp.float32),
            pltpu.VMEM((count, count), jnp.float32),
            pltpu.VMEM((together, count, count), jnp.float32),
            pltpu.VMEM((deep, count), jnp.float32),
            pltpu.VMEM((count, deep), jnp.bfloat16),
            pltpu.SemaphoreType.DMA((9,)),
        ],
        compiler_params=PARAMS,
        cost_estimate=cost(0.025 * count),
        name="mix_frames",
    )(frame, *[part.reshape(shape) for part in gathered], *in_hbm(weight, *after))
    return mixed.reshape(whole, share, attended)


def finish_kernel(
    first, delta, residual_far, mixed, weight, modulation, gain, out_weight, latents, *refs,
):
    hidden_far, velocity_far, update_far, residual, hidden, velocity, update, sems = refs[-8:]
    blocks = residual.shape[0] // QUERY_BLOCK
    loads = start_all(
        [
            pltpu.make_async_copy(
                residual_far.at[pl.ds(block * QUERY_BLOCK, QUERY_BLOCK), :],
                residual.at[pl.ds(block * QUERY_BLOCK, QUERY_BLOCK), :],
                sems.at[2 + blocks + block],
            )
            for block in range(blocks)
        ]
    )
    count, width = residual.shape
    channels = out_weight.shape[0]
    fold = LANES // channels
    lines = pl.ds(first // fold, count // fold)
    spread = lax.rem(lax.broadcasted_iota(jnp.int32, (LANES, channels), 0), channels)
    spread = jnp.where(
        spread == lax.broadcasted_iota(jnp.int32, (LANES, channels), 1), 1.0, 0.0
    ).astype(jnp.bfloat16)
    repeated = jnp.dot(spread, out_weight[...], preferred_element_type=jnp.float32)
    repeated = repeated.astype(jnp.bfloat16)
    stores = []
    for start in range(0, count, QUERY_BLOCK):
        span = slice(start, start + QUERY_BLOCK)
        term = jnp.dot(mixed[span, :], weight[...], preferred_element_type=jnp.float32)
        loads[start // QUERY_BLOCK].wait()
        block = residual[span, :] + modulation[:, 2 * width :] * term
        hidden[span, :] = block.astype(jnp.bfloat16)
        copy = pltpu.make_async_copy(
            hidden.at[pl.ds(start, QUERY_BLOCK), :],
            hidden_far.at[pl.ds(first + start, QUERY_BLOCK), :],
            sems.at[2 + len(stores)],
        )
        copy.start()
        stores.append(copy)
        final_rows = (normalized(block) * gain[...]).astype(jnp.bfloat16)
        wide = lax.dot_general(final_rows, repeated, ACROSS, preferred_element_type=jnp.float32)
        row = lax.rem(lax.broadcasted_iota(jnp.int32, (QUERY_BLOCK, LANES), 0), fold)
        lane = lax.broadcasted_iota(jnp.int32, (QUERY_BLOCK, LANES), 1) // channels
        picked = jnp.where(row == lane, wide, 0.0).reshape(QUERY_BLOCK // fold, fold, LANES)
        velocity[start // fold : (start + QUERY_BLOCK) // fold, :] = jnp.sum(picked, axis=1)
    known = latents[first // fold : (first + count) // fold, :]
    update[...] = (known + delta[...] * velocity[...]).astype(jnp.bfloat16)
    stores += start_all(
        [
            pltpu.make_async_copy(velocity, velocity_far.at[lines, :], sems.at[0]),
            pltpu.make_async_copy(update, update_far.at[lines, :], sems.at[1]),
        ]
    )
    for copy in stores:
        copy.wait()


def finish(first, so_far, delta, residual, mixed, weight, modulation, gain, out_weight, latents, tokens):
    count, width = residual.shape
    lines = count * out_weight.shape[0] // LANES
    known = 8
    (residual,) = in_hbm(residual)
    return pl.pallas_call(
        functools.partial(finish_kernel, first),
        out_shape=(
            pltpu.HBM((tokens, width), jnp.bfloat16),
            pltpu.HBM(latents.shape, jnp.float32),
            pltpu.HBM(latents.shape, jnp.bfloat16),
        ),
        in_specs=[WHOLE, REMAIN] + [WHOLE] * 6 + [REMAIN] * len(so_far),
        out_specs=(REMAIN,) * 3,
        scratch_shapes=[
            pltpu.VMEM((count, width), jnp.float32),
            pltpu.VMEM((count, width), jnp.bfloat16),
            pltpu.VMEM((lines, LANES), jnp.float32),
            pltpu.VMEM((lines, LANES), jnp.bfloat16),
            pltpu.SemaphoreType.DMA((2 + 2 * (count // QUERY_BLOCK),)),
        ],
        input_output_aliases={known + place: place for place in range(len(so_far))},
        compiler_params=PARAMS,
        cost_estimate=cost(0.012 * count),
        name="finish",
    )(delta, residual, mixed, weight, modulation, gain, out_weight, latents, *so_far)


FIRST_BLOCKS = 1
PERMUTED = (1,)


def chunks_of(tokens, peers):
    least = round_up(QUERY_BLOCK, 16 * peers)
    head = FIRST_BLOCKS * least
    if least % QUERY_BLOCK or tokens % least or head >= tokens:
        return [(0, tokens)]
    return [(0, head), (head, tokens - head)]


def by_permutes(place, peers):
    return place in PERMUTED and peers & (peers - 1) == 0


def exchange(parts, peers):
    if len(parts) == 1:
        return [lax.all_to_all(parts[0], "frame", 0, 0, tiled=True)]
    arrived = list(parts)
    for slot in reversed(range(1, peers)):
        pairs = [(index, index ^ slot) for index in range(peers)]
        arrived[slot] = lax.ppermute(parts[slot], "frame", pairs)
    return arrived


def steps(
    hidden_in,
    latents,
    fresh_noise,
    level_index,
    time_table,
    frame_offset,
    mod_table,
    time_weight,
    spatial_qkv,
    spatial_out,
    temporal_qkv,
    temporal_out,
    final_gain,
    out_weight,
):
    tokens = hidden_in.shape[1]
    attended = spatial_out.shape[0]
    head_count = attended // HEAD_SIZE
    peers = lax.axis_size("frame")
    hidden = hidden_in[0]
    frame = lax.axis_index("frame").astype(jnp.int32).reshape(1)
    spatial_turned = jnp.transpose(spatial_qkv)
    temporal_turned = jnp.transpose(temporal_qkv)
    keys, values, normed, modulation, placed, delta = keys_and_values(
        level_index, time_table, frame_offset, frame, hidden, mod_table.reshape(-1, LANES),
        time_weight, spatial_turned, head_count,
    )
    swap = [(0, 1), (1, 0)]
    other = (lax.ppermute(keys, "band", swap), lax.ppermute(values, "band", swap))
    queries = project_queries(normed, spatial_turned, head_count)
    chunks = chunks_of(tokens, peers)
    residuals, gathered = [], []
    for place, (first, size) in enumerate(chunks):
        slots = peers if by_permutes(place, peers) else 0
        residual, *temporal_in = attend(
            first, size, first == 0, slots, frame, hidden, (queries, keys, values), other,
            spatial_out, modulation, placed,
        )
        residuals.append(residual)
        if slots:
            temporal_in = [part[None] for part in temporal_in]
        else:
            temporal_in = [temporal_in[0].reshape(peers, size // peers, -1)]
        gathered.append(exchange(temporal_in, peers))
    last = residuals[-1]
    returned = []
    for parts in gathered:
        mixed = mix_frames(frame, parts, temporal_turned, attended, (last,))
        returned.append(exchange([mixed], peers)[0])
    so_far = ()
    for (first, _), residual, mixed in zip(chunks, residuals, returned):
        so_far = finish(
            first, so_far, delta, residual, mixed.reshape(-1, attended), temporal_out,
            modulation, final_gain[None, :], jnp.transpose(out_weight), latents[0], tokens,
        )
    hidden_out, velocity, update = so_far
    shifted = from_behind(update, "frame", 1).astype(jnp.float32)[None]
    next_latents = jnp.where(lax.axis_index("frame") == 0, fresh_noise[None], shifted)
    return (hidden_out[None], velocity[None], next_latents)


def solution(mesh):
    placed = (
        P(("groups", "frame"), "band", None),
        P(("groups", "frame"), "band", None),
        P(("groups", "band"), None),
        P(("groups", "frame")),
        P(),
        P("groups"),
        P(),
        P(),
        P(),
        P(),
        P(),
        P(),
        P(),
        P(),
    )
    return jax.shard_map(
        steps,
        mesh=mesh,
        in_specs=placed,
        out_specs=(
            P(("groups", "frame"), "band", None),
            P(("groups", "frame"), "band", None),
            P(("groups", "frame"), "band", None),
        ),
        check_vma=False,
    )
```
